256 devices in a mesh: gx: 4 (over z_hi), gy: 16 (over z_lo, x, core), gz: 4 (over y).
Axes of the slice: x: 4, y: 4, z: 8 (z_hi: 4, z_lo: 2; z = z_hi * 2 + z_lo), core: 2. Of those that a mesh axis runs over, the one named last changes fastest.
Arguments:
- fields: bfloat16 [5, 128, 768, 512], P(None, 'gx', 'gy', 'gz'), may hold values from -8 to 8
Outputs:
- filtered: bfloat16 [5, 128, 768, 512], P(None, 'gx', 'gy', 'gz')
- stress: bfloat16 [15, 128, 768, 512], P(None, 'gx', 'gy', 'gz')
The draws below stay inside these ranges and needn't reach their ends.
All inputs are finite; a program needn't handle non-finite values.
Results may differ from the reference program's by a relative error of at most 0.0022.
Values may be sent and summed in bfloat16 or wider, within the bound.
No kernel may reach another device: no remote copies, remote signals or barrier semaphores. Data moves between devices by JAX's collectives and lax.ppermute only.
A program may use at most 128 MiB of HBM per device.

```python
import jax
import jax.numpy as jnp
from jax import lax

R = 32
NX = 128
NY = 768
NZ = 512


def block_index(count):
    return (jnp.arange(count, dtype=jnp.int32) // 16).astype(jnp.int32)


def block_count(count):
    return (count + 15) // 16


def coarse_noise(key, shape):
    return jax.random.normal(key, shape, jnp.float32) * 0.9


def draw_fields(key, part):
    keys = jax.random.split(jax.random.fold_in(key, 17), 11)
    coord_x = (jnp.arange(NX, dtype=jnp.float32) + 0.5) / NX
    coord_y = jnp.arange(NY, dtype=jnp.float32) / NY
    coord_z = jnp.arange(NZ, dtype=jnp.float32) / NZ
    mixing = jax.random.normal(keys[0], (5, 5), jnp.float32) * 0.35 + jnp.eye(5, dtype=jnp.float32) * 0.8
    means = jax.random.uniform(keys[1], (5,), jnp.float32, -0.4, 0.4)
    jumps = jax.random.uniform(keys[2], (5,), jnp.float32, 0.2, 0.5)
    phases = jax.random.uniform(keys[3], (2,), jnp.float32, 0.0, 1.0)
    front = 0.5 + 0.12 * jnp.sin(2.0 * jnp.pi * (2.0 * coord_y[:, None] + phases[0])) + 0.08 * jnp.sin(2.0 * jnp.pi * (3.0 * coord_z[None, :] + phases[1]))
    distance = coord_x[:, None, None] - front[None, :, :]
    profile = jnp.tanh(distance / 0.08)
    envelope = 0.3 + 0.7 * jnp.exp(-(distance / 0.15) ** 2)
    line_x = jax.random.normal(keys[4], (5, NX + 1), jnp.float32)
    line_y = jax.random.normal(keys[5], (5, NY + 1), jnp.float32)
    line_z = jax.random.normal(keys[6], (5, NZ + 1), jnp.float32)
    bulk = jax.random.normal(keys[7], (5, NX, NY, NZ), jnp.float32)
    index_x = block_index(NX)
    index_y = block_index(NY)
    index_z = block_index(NZ)
    coarse_a = coarse_noise(keys[8], (5, NX, block_count(NY), block_count(NZ)))
    coarse_b = coarse_noise(keys[9], (5, block_count(NX), NY, block_count(NZ)))
    coarse_c = coarse_noise(keys[10], (5, block_count(NX), block_count(NY), NZ))
    white_x = jnp.take(jnp.take(coarse_a, index_y, axis=2), index_z, axis=3)
    white_y = jnp.take(jnp.take(coarse_b, index_x, axis=1), index_z, axis=3)
    white_z = jnp.take(jnp.take(coarse_c, index_x, axis=1), index_y, axis=2)
    step_x = (line_x[:, 1:] - line_x[:, :-1]) * 0.6
    step_y = (line_y[:, 1:] - line_y[:, :-1]) * 0.6
    step_z = (line_z[:, 1:] - line_z[:, :-1]) * 0.6
    rough = step_x[:, :, None, None] + step_y[:, None, :, None] + step_z[:, None, None, :] + 0.4 * envelope[None] * bulk + white_x + white_y + white_z
    mixed = jnp.einsum('cd,dxyz->cxyz', mixing, rough)
    values = means[:, None, None, None] + jumps[:, None, None, None] * profile[None] + mixed
    return jnp.clip(values, -8.0, 8.0).astype(jnp.bfloat16)


def setup_inputs(seed: int = 0) -> dict:
    splits = jax.random.split(jax.random.key(seed), 2)
    return {
        "fields": draw_fields(jax.random.fold_in(splits[1], 71), 0),
    }


pair_first = (0, 0, 0, 0, 0, 1, 1, 1, 1, 2, 2, 2, 3, 3, 4)
pair_second = (0, 1, 2, 3, 4, 1, 2, 3, 4, 2, 3, 4, 3, 4, 4)


def taps(offset):
    return jnp.where(jnp.abs(offset) <= R, 1.0, 0.0).astype(jnp.bfloat16)


def edge_norm(count, whole):
    cells = jnp.arange(count, dtype=jnp.int32)[:, None]
    offsets = jnp.arange(-R, R + 1, dtype=jnp.int32)[None, :]
    inside = (cells + offsets >= 0) & (cells + offsets < whole)
    return jnp.sum(jnp.where(inside, taps(offsets).astype(jnp.float32), 0.0), axis=1)


def reference(fields):
    offsets = jnp.arange(-R, R + 1, dtype=jnp.int32)
    weights = lax.optimization_barrier(taps(offsets)).astype(jnp.float32)
    total = jnp.sum(weights)
    norm_x = edge_norm(NX, NX)[:, None, None]

    def kernel(length):
        index = ((-offsets) % length).astype(jnp.int32)
        return jnp.zeros((length,), jnp.float32).at[index].add(weights)

    def along(values, axis, length):
        count = values.shape[axis]
        spectrum = jnp.fft.rfft(values, n=length, axis=axis)
        shape = [1, 1, 1]
        shape[axis] = -1
        factor = jnp.fft.rfft(kernel(length)).reshape(shape)
        result = jnp.fft.irfft(spectrum * factor, n=length, axis=axis)
        return lax.slice_in_dim(result, 0, count, axis=axis)

    def smooth_one(block):
        first = (along(block.astype(jnp.float32), 0, NX + 2 * R) / norm_x).astype(jnp.bfloat16)
        first = lax.optimization_barrier(first).astype(jnp.float32)
        second = (along(first, 2, NZ) / total).astype(jnp.bfloat16)
        second = lax.optimization_barrier(second).astype(jnp.float32)
        return along(second, 1, NY) / total

    smooth_fields = lax.map(smooth_one, fields)
    first_table = jnp.array(pair_first, jnp.int32)
    second_table = jnp.array(pair_second, jnp.int32)

    def pair_one(pair):
        left_index = first_table[pair]
        right_index = second_table[pair]
        left = lax.dynamic_index_in_dim(fields, left_index, 0, keepdims=False)
        right = lax.dynamic_index_in_dim(fields, right_index, 0, keepdims=False)
        product = (left.astype(jnp.float32) * right.astype(jnp.float32)).astype(jnp.bfloat16)
        smooth = smooth_one(product)
        mean_left = lax.dynamic_index_in_dim(smooth_fields, left_index, 0, keepdims=False)
        mean_right = lax.dynamic_index_in_dim(smooth_fields, right_index, 0, keepdims=False)
        return (smooth - mean_left * mean_right).astype(jnp.bfloat16)

    stress = lax.map(pair_one, jnp.arange(15, dtype=jnp.int32))
    return smooth_fields.astype(jnp.bfloat16), stress
```

```python
import jax
import jax.numpy as jnp
from jax import lax
from jax.experimental import pallas as pl
from jax.experimental.pallas import tpu as pltpu
from jax.sharding import PartitionSpec as P

R = 32
pair_first = (0, 0, 0, 0, 0, 1, 1, 1, 1, 2, 2, 2, 3, 3, 4)
pair_second = (0, 1, 2, 3, 4, 1, 2, 3, 4, 2, 3, 4, 3, 4, 4)
H = 16
F32 = jnp.float32
BF16 = jnp.bfloat16


def components(ref, x):
    values = [ref[c, x] for c in range(5)]
    values += [values[a] * values[b] for a, b in zip(pair_first, pair_second)]
    return [v.astype(F32) for v in values]


def stream_kernel(inv_ref, lo_ref, own_ref, hi_ref, pack_ref, out_ref, low_ref, high_ref, acc_ref):
    step = pl.program_id(0)

    @pl.when(step == 0)
    def _():
        def add(x, acc):
            lo = components(lo_ref, x)
            own = components(own_ref, x)
            return tuple(a + (b + c) for a, b, c in zip(acc, lo, own))

        acc = lax.fori_loop(0, 32, add, tuple(jnp.zeros((H, 128), F32) for _ in range(20)))
        for c in range(20):
            acc_ref[c] = acc[c]

    def slide(i, acc):
        x = step * 8 + i
        inv = inv_ref[x]
        hi = components(hi_ref, x)
        acc = [a + b for a, b in zip(acc, hi)]
        for c in range(20):
            out_ref[c, i] = (acc[c] * inv).astype(BF16)
        lo = components(lo_ref, x)
        return tuple(a - b for a, b in zip(acc, lo))

    acc = lax.fori_loop(0, 8, slide, tuple(acc_ref[c] for c in range(20)))
    for c in range(20):
        acc_ref[c] = acc[c]
    for s in range(2):
        rows = jnp.concatenate([out_ref[:, 4 * s + q].reshape(20 * H, 128) for q in range(4)], axis=1)
        packed = jnp.dot(rows, pack_ref[...], preferred_element_type=F32).astype(BF16)
        low_ref[:, s] = packed[:, :128].reshape(20, H, 128)
        high_ref[:, s] = packed[:, 128:].reshape(20, H, 128)


def stream_filter(inv, lo, own, hi, pack):
    whole = pl.BlockSpec((5, 32, H, 128), lambda b: (0, 0, 0, 0))
    return pl.pallas_call(
        stream_kernel,
        grid=(4,),
        in_specs=[
            pl.BlockSpec(memory_space=pltpu.SMEM),
            whole,
            whole,
            whole,
            pl.BlockSpec((512, 256), lambda b: (0, 0)),
        ],
        out_specs=[
            pl.BlockSpec((20, 8, H, 128), lambda b: (0, b, 0, 0)),
            pl.BlockSpec((20, 2, H, 128), lambda b: (0, b, 0, 0)),
            pl.BlockSpec((20, 2, H, 128), lambda b: (0, b, 0, 0)),
        ],
        out_shape=[
            jax.ShapeDtypeStruct((20, 32, H, 128), BF16),
            jax.ShapeDtypeStruct((20, 8, H, 128), BF16),
            jax.ShapeDtypeStruct((20, 8, H, 128), BF16),
        ],
        scratch_shapes=[pltpu.VMEM((20, H, 128), F32)],
        name="stream_filter",
    )(inv, lo, own, hi, pack)


def trans_kernel(own_ref, low_ref, high_ref, band_ref, out_ref):
    low = low_ref[...].reshape(4 * 8 * H, 128)
    high = high_ref[...].reshape(4 * 8 * H, 128)
    for h in range(2):
        rows = jnp.concatenate(
            [own_ref[:, :, 2 * h].reshape(4 * 8 * H, 128), own_ref[:, :, 2 * h + 1].reshape(4 * 8 * H, 128), low, high],
            axis=1,
        )
        result = jnp.dot(rows, band_ref[h], preferred_element_type=F32) * (1.0 / (2 * R + 1))
        result = result.astype(BF16)
        for e in range(2):
            out_ref[:, :, 2 * h + e] = result[:, 128 * e : 128 * e + 128].reshape(4, 8, H, 128)


def trans_filter(own, low, high, band):
    own = own.reshape(20, 8, 4, H, 128)
    out = pl.pallas_call(
        trans_kernel,
        grid=(5,),
        in_specs=[
            pl.BlockSpec((4, 8, 4, H, 128), lambda b: (b, 0, 0, 0, 0)),
            pl.BlockSpec((4, 8, H, 128), lambda b: (b, 0, 0, 0)),
            pl.BlockSpec((4, 8, H, 128), lambda b: (b, 0, 0, 0)),
            pl.BlockSpec((2, 512, 256), lambda b: (0, 0, 0)),
        ],
        out_specs=pl.BlockSpec((4, 8, 4, H, 128), lambda b: (b, 0, 0, 0, 0)),
        out_shape=jax.ShapeDtypeStruct((20, 8, 4, H, 128), BF16),
        name="trans_filter",
    )(own, low, high, band)
    return out.reshape(20, 32, H, 128)


def span_kernel(band_ref, *refs):
    pieces, (filtered_ref, stress_ref) = refs[:7], refs[7:]
    band = band_ref[...]
    scale = 1.0 / (2 * R + 1)
    for x in range(0, 4, 2):

        def smooth(c):
            rows = jnp.concatenate(
                [jnp.concatenate([ref[c, x + e] for ref in pieces], axis=0) for e in range(2)], axis=1
            )
            return jnp.dot(band, rows, preferred_element_type=F32) * scale

        means = [smooth(c) for c in range(5)]
        for c in range(5):
            for e in range(2):
                filtered_ref[c, x + e] = means[c][:, 128 * e : 128 * e + 128].astype(BF16)
        for p in range(15):
            result = smooth(5 + p) - means[pair_first[p]] * means[pair_second[p]]
            for e in range(2):
                stress_ref[p, x + e] = result[:, 128 * e : 128 * e + 128].astype(BF16)


def span_filter(band, pieces):
    rows = 3 * H
    return pl.pallas_call(
        span_kernel,
        grid=(8,),
        in_specs=[pl.BlockSpec((rows, 7 * H), lambda b: (0, 0))]
        + [pl.BlockSpec((20, 4, H, 128), lambda b: (0, b, 0, 0))] * 7,
        out_specs=[
            pl.BlockSpec((5, 4, rows, 128), lambda b: (0, b, 0, 0)),
            pl.BlockSpec((15, 4, rows, 128), lambda b: (0, b, 0, 0)),
        ],
        out_shape=[
            jax.ShapeDtypeStruct((5, 32, rows, 128), BF16),
            jax.ShapeDtypeStruct((15, 32, rows, 128), BF16),
        ],
        name="span_filter",
    )(band, *pieces)


def iota(shape, dim):
    return lax.broadcasted_iota(jnp.int32, shape, dim)


def inverse_norm(start, count, whole):
    cells = start + jnp.arange(count, dtype=jnp.int32)
    inside = jnp.minimum(cells + R, whole - 1) - jnp.maximum(cells - R, 0) + 1
    return 1.0 / inside.astype(F32)


def pack_matrix():
    k, n = iota((512, 256), 0), iota((512, 256), 1)
    group, lane = k // 128, k % 128
    side, target = n // 128, n % 128
    return ((target // 32 == group) & (lane == target % 32 + 96 * side)).astype(BF16)


def trans_band():
    shape = (2, 512, 256)
    h, k, n = iota(shape, 0), iota(shape, 1), iota(shape, 2)
    part, lane = k // 128, k % 128
    e, target = n // 128, n % 128
    own = (part == e) & (jnp.abs(lane - target) <= R)
    mine = lane // 32 == 2 * h + e
    low = (part == 2) & mine & (jnp.abs(lane % 32 - 32 - target) <= R)
    high = (part == 3) & mine & (jnp.abs(lane % 32 + 128 - target) <= R)
    return (own | low | high).astype(BF16)


def span_band(odd, depth):
    inner = [jnp.where(odd, depth - H * (k + 1), H * k) for k in range(3)]
    outer = [jnp.where(odd, depth + H * k, -H * (k + 1)) for k in range(2)]
    across = [jnp.where(odd, H * k - depth, 2 * depth - H * (k + 1)) for k in (1, 2)]
    starts = jnp.stack(inner + outer + across)
    position = (starts[:, None] + jnp.arange(H, dtype=jnp.int32)[None, :]).reshape(1, 7 * H)
    rows = iota((depth, 7 * H), 0)
    return (jnp.abs(position - rows) <= R).astype(BF16)


def body(fields):
    depth_x, depth_y = fields.shape[1], fields.shape[2]
    nx, ny, nz = lax.axis_size("gx"), lax.axis_size("gy"), lax.axis_size("gz")
    odd = lax.axis_index("gy") % 2 == 1
    inv = inverse_norm(lax.axis_index("gx") * depth_x, depth_x, depth_x * nx)
    pack, band_z, band_y = pack_matrix(), trans_band(), span_band(odd, depth_y)
    forward_x = [(i, i + 1) for i in range(nx - 1)]
    backward_x = [(i + 1, i) for i in range(nx - 1)]
    forward_z = [(i, (i + 1) % nz) for i in range(nz)]
    backward_z = [((i + 1) % nz, i) for i in range(nz)]
    off_chip = [(i, (i - 1) % ny if i % 2 == 0 else (i + 1) % ny) for i in range(ny)]
    on_chip = [(i, i + 1 if i % 2 == 0 else i - 1) for i in range(ny)]

    blocks, lows, highs = [], [], []
    for k in range(3):
        start = jnp.where(odd, depth_y - H * (k + 1), H * k)
        block = lax.dynamic_slice_in_dim(fields, start, H, axis=2)
        blocks.append(block)
        lows.append(lax.ppermute(block, "gx", forward_x))
        highs.append(lax.ppermute(block, "gx", backward_x))

    own, outer, across = [], [], []
    for k in range(3):
        streamed, low, high = stream_filter(inv, lows[k], blocks[k], highs[k], pack)
        from_low = lax.ppermute(high, "gz", forward_z)
        from_high = lax.ppermute(low, "gz", backward_z)
        done = trans_filter(streamed, from_low, from_high, band_z)
        own.append(done)
        if k < 2:
            outer.append(lax.ppermute(done, "gy", off_chip))
        if k > 0:
            across.append(lax.ppermute(done, "gy", on_chip))
    return tuple(span_filter(band_y, own + outer + across))


def solution(mesh):
    spec = P(None, "gx", "gy", "gz")
    return jax.shard_map(body, mesh=mesh, in_specs=(spec,), out_specs=(spec, spec), check_vma=False)
```

```python
import jax
import jax.numpy as jnp
import numpy as np
from jax import lax
from jax.experimental import pallas as pl
from jax.experimental.pallas import tpu as pltpu
from jax.sharding import PartitionSpec as P


R = 32
pair_first = (0, 0, 0, 0, 0, 1, 1, 1, 1, 2, 2, 2, 3, 3, 4)
pair_second = (0, 1, 2, 3, 4, 1, 2, 3, 4, 2, 3, 4, 3, 4, 4)
SCALE = 1.0 / (2 * R + 1)
H = 8
GROUPS = ((0,), (1,), (2,), (3,), (4,), (5,))
WINDOW = 2
F32 = jnp.float32
BF16 = jnp.bfloat16


VMEM = pl.BlockSpec(memory_space=pltpu.VMEM)
SMEM = pl.BlockSpec(memory_space=pltpu.SMEM)


def held(*arrays):
    return tuple(pltpu.with_memory_space_constraint(a, pltpu.VMEM) for a in arrays)


def components(ref, g, p, mask=None):
    values = [ref[g, c, p] for c in range(5)]
    if mask is not None:
        values = [v * mask for v in values]
    values += [values[a] * values[b] for a, b in zip(pair_first, pair_second)]
    return [v.astype(F32) for v in values]


def stream_kernel(inv_ref, edge_ref, lo_ref, own_ref, hi_ref, pack_ref, out_ref, low_ref, high_ref):
    mask_lo = jnp.full((2 * H, 128), edge_ref[0], F32).astype(BF16)
    mask_hi = jnp.full((2 * H, 128), edge_ref[1], F32).astype(BF16)

    @pl.loop(0, own_ref.shape[0])
    def _(g):
        def add(p, acc):
            lo = components(lo_ref, g, p, mask_lo)
            own = components(own_ref, g, p)
            both = [a + b for a, b in zip(lo, own)]
            return tuple(a + (b[:H] + b[H:]) for a, b in zip(acc, both))

        acc = lax.fori_loop(0, 16, add, tuple(jnp.zeros((H, 128), F32) for _ in range(20)))

        def slide(p, acc):
            inv_a, inv_b = inv_ref[2 * p], inv_ref[2 * p + 1]
            hi = components(hi_ref, g, p, mask_hi)
            lo = components(lo_ref, g, p, mask_lo)
            result = []
            for c in range(20):
                first = acc[c] + hi[c][:H]
                second = first + (hi[c][H:] - lo[c][:H])
                result.append(second - lo[c][H:])
                out_ref[g, c, p] = jnp.concatenate([first * inv_a, second * inv_b], axis=0).astype(BF16)
            return tuple(result)

        lax.fori_loop(0, 16, slide, acc)

        @pl.loop(0, 5)
        def _(b):
            part = pl.ds(4 * b, 4)
            block = out_ref[g, part].reshape(4, 4, 4, 2 * H, 128)
            rows = jnp.concatenate([block[:, :, q].reshape(32 * H, 128) for q in range(4)], axis=1)
            packed = jnp.dot(rows, pack_ref[...], preferred_element_type=F32).astype(BF16)
            low_ref[g, part] = packed[:, :128].reshape(4, 4, 2 * H, 128)
            high_ref[g, part] = packed[:, 128:].reshape(4, 4, 2 * H, 128)


def stream_filter(inv, edge, lo, own, hi, pack):
    n = own.shape[0]
    return pl.pallas_call(
        stream_kernel,
        in_specs=[SMEM, SMEM, VMEM, VMEM, VMEM, VMEM],
        out_specs=[VMEM, VMEM, VMEM],
        out_shape=[
            pltpu.VMEM((n, 20, 16, 2 * H, 128), BF16),
            pltpu.VMEM((n, 20, 4, 2 * H, 128), BF16),
            pltpu.VMEM((n, 20, 4, 2 * H, 128), BF16),
        ],
        compiler_params=pltpu.CompilerParams(vmem_limit_bytes=6 << 20),
        name="stream_filter",
    )(inv, edge, *held(lo, own, hi, pack))


def trans_kernel(own_ref, low_ref, high_ref, band_ref, out_ref):
    @pl.loop(0, own_ref.shape[0])
    def _(g):
        @pl.loop(0, 5)
        def _(b):
            part = pl.ds(4 * b, 4)
            own = own_ref[g, part].reshape(4, 4, 4, 2 * H, 128)
            low = low_ref[g, part].reshape(32 * H, 128)
            high = high_ref[g, part].reshape(32 * H, 128)
            for h in range(2):
                rows = jnp.concatenate(
                    [own[:, :, 2 * h].reshape(32 * H, 128), own[:, :, 2 * h + 1].reshape(32 * H, 128), low, high],
                    axis=1,
                )
                result = jnp.dot(rows, band_ref[h], preferred_element_type=F32) * SCALE
                result = result.astype(BF16).reshape(4, 4, 2 * H, 256)
                for s in range(4):
                    for e in range(2):
                        out_ref[g, part, 4 * s + 2 * h + e] = result[:, s, :, 128 * e : 128 * e + 128]


def trans_filter(own, low, high, band):
    return pl.pallas_call(
        trans_kernel,
        in_specs=[VMEM] * 4,
        out_specs=VMEM,
        out_shape=pltpu.VMEM(own.shape, BF16),
        compiler_params=pltpu.CompilerParams(vmem_limit_bytes=6 << 20),
        name="trans_filter",
    )(*held(own, low, high, band))


def span_kernel(band_ref, *refs):
    pieces, (filtered_ref, stress_ref, filtered_buf, stress_buf, sems) = refs[:-5], refs[-5:]
    rows = filtered_buf.shape[3]
    order = [(ref, g) for ref in pieces for g in range(ref.shape[0])]

    def copies(step, slot):
        x = step * 4
        return (
            pltpu.make_async_copy(filtered_buf.at[slot], filtered_ref.at[:, pl.ds(x, 4)], sems.at[0, slot]),
            pltpu.make_async_copy(stress_buf.at[slot], stress_ref.at[:, pl.ds(x, 4)], sems.at[1, slot]),
        )

    def step_body(step, _):
        slot = lax.rem(step, 2)

        @pl.when(step >= 2)
        def _():
            for copy in copies(step - 2, slot):
                copy.wait()

        def smooth(c):
            tile = jnp.concatenate(
                [jnp.concatenate([ref[g, c, 2 * step + i] for ref, g in order], axis=0) for i in range(2)], axis=1
            )
            return jnp.dot(band_ref[...], tile, preferred_element_type=F32) * SCALE

        def put(buf, c, value):
            for i in range(2):
                for e in range(2):
                    buf[slot, c, 2 * i + e] = value[rows * e : rows * e + rows, 128 * i : 128 * i + 128].astype(BF16)

        means = [smooth(c) for c in range(5)]
        for c in range(5):
            put(filtered_buf, c, means[c])
        for p in range(15):
            put(stress_buf, p, smooth(5 + p) - means[pair_first[p]] * means[pair_second[p]])
        for copy in copies(step, slot):
            copy.start()
        return 0

    lax.fori_loop(0, 8, step_body, 0)
    for step in (6, 7):
        for copy in copies(step, step % 2):
            copy.wait()


def span_filter(band, pieces, depth):
    anywhere = pl.BlockSpec(memory_space=pl.ANY)
    return pl.pallas_call(
        span_kernel,
        in_specs=[VMEM] * (1 + len(pieces)),
        out_specs=[anywhere, anywhere],
        out_shape=[
            jax.ShapeDtypeStruct((5, 32, depth, 128), BF16),
            jax.ShapeDtypeStruct((15, 32, depth, 128), BF16),
        ],
        scratch_shapes=[
            pltpu.VMEM((2, 5, 4, depth, 128), BF16),
            pltpu.VMEM((2, 15, 4, depth, 128), BF16),
            pltpu.SemaphoreType.DMA((2, 2)),
        ],
        compiler_params=pltpu.CompilerParams(vmem_limit_bytes=8 << 20),
        name="span_filter",
    )(*held(band, *pieces))


def inverse_norm(start, count, whole):
    cells = start + jnp.arange(count, dtype=jnp.int32)
    inside = jnp.minimum(cells + R, whole - 1) - jnp.maximum(cells - R, 0) + 1
    return 1.0 / inside.astype(F32)


def pack_matrix():
    k, n = np.indices((512, 256))
    return jnp.asarray((n % 128 // 32 == k // 128) & (k % 128 == n % 32 + 96 * (n // 128)), BF16)


def trans_band():
    h, k, n = np.indices((2, 512, 256))
    part, lane, e, target = k // 128, k % 128, n // 128, n % 128
    own = (part == e) & (np.abs(lane - target) <= R)
    mine = lane // 32 == 2 * h + e
    low = (part == 2) & mine & (np.abs(lane % 32 - 32 - target) <= R)
    high = (part == 3) & mine & (np.abs(lane % 32 + 128 - target) <= R)
    return jnp.asarray(own | low | high, BF16)


def span_band(odd, depth, outer, across):
    bands = []
    count = depth // H
    for core in range(2):
        starts = [depth - H * (k + 1) if core else H * k for k in range(count)]
        starts += [depth + H * k if core else -H * (k + 1) for k in outer]
        starts += [H * k - depth if core else 2 * depth - H * (k + 1) for k in across]
        position = np.array(starts)[:, None, None] + np.zeros((1, 2, 1), int) + np.arange(H)[None, None, :]
        half = np.zeros((len(starts), 1, 1), int) + np.arange(2)[None, :, None] + np.zeros((1, 1, H), int)
        position, half = position.reshape(1, -1), half.reshape(1, -1)
        e, row = np.indices((2, depth))
        e, row = e.reshape(-1, 1), row.reshape(-1, 1)
        bands.append((e == half) & (np.abs(position - row) <= R))
    return jnp.where(odd, jnp.asarray(bands[1], BF16), jnp.asarray(bands[0], BF16))


def plan(fields):
    depth_x, depth_y = fields.shape[1], fields.shape[2]
    nx, ny, nz = lax.axis_size("gx"), lax.axis_size("gy"), lax.axis_size("gz")
    place = lax.axis_index("gx")
    odd = lax.axis_index("gy") % 2 == 1
    inv = inverse_norm(place * depth_x, depth_x, depth_x * nx)
    edge = jnp.stack([place > 0, place < nx - 1]).astype(F32)
    outer_pieces = [k for group in GROUPS for k in group if k < 4]
    across_pieces = [k for group in GROUPS for k in group if k >= 2]
    pack, band_z = pack_matrix(), trans_band()
    band_y = span_band(odd, depth_y, outer_pieces, across_pieces)

    def ring(n, by):
        return [(i, (i + by) % n) for i in range(n)]

    off_chip = [(i, (i - 1) % ny if i % 2 == 0 else (i + 1) % ny) for i in range(ny)]
    on_chip = [(i, i + 1 if i % 2 == 0 else i - 1) for i in range(ny)]

    def after(value, *others):
        return lax.optimization_barrier((value, *others))[0]

    count = len(GROUPS)
    blocks, lows, highs = [], [], []

    def send_x(i, *others):
        parts = []
        for k in GROUPS[i]:
            start = jnp.where(odd, depth_y - H * (k + 1), H * k)
            part = lax.dynamic_slice_in_dim(fields, start, H, axis=2)
            parts.append(part.reshape(1, 5, 16, 2 * H, 128))
        block = jnp.concatenate(parts, axis=0)
        blocks.append(block)
        ahead = behind = block
        if i >= WINDOW:
            ahead = after(block, lows[i - WINDOW], *others)
            behind = after(block, highs[i - WINDOW], *others)
        lows.append(lax.ppermute(ahead, "gx", ring(nx, 1)))
        highs.append(lax.ppermute(behind, "gx", ring(nx, -1)))

    own, outer, across, waiting = [], [], [], []

    def finish_z(i, *others):
        streamed, from_low, from_high = waiting[i]
        streamed = after(streamed, *others)
        done = trans_filter(streamed, from_low, from_high, band_z)
        own.append(done)
        if max(GROUPS[i]) < 4:
            outer.append(lax.ppermute(done, "gy", off_chip))
        if min(GROUPS[i]) >= 2:
            across.append(lax.ppermute(done, "gy", on_chip))

    for i in range(WINDOW):
        send_x(i)
    for i in range(count):
        last = own[-1:]
        if i + WINDOW < count:
            send_x(i + WINDOW, *last)
        streamed, low, high = stream_filter(inv, edge, lows[i], after(blocks[i], *last), highs[i], pack)
        from_low = lax.ppermute(high, "gz", ring(nz, 1))
        from_high = lax.ppermute(low, "gz", ring(nz, -1))
        waiting.append((streamed, from_low, from_high))
        if i > 0:
            finish_z(i - 1, streamed)
    finish_z(count - 1)
    return tuple(span_filter(band_y, own + outer + across, depth_y))


def solution(mesh):
    spec = P(None, "gx", "gy", "gz")
    return jax.shard_map(plan, mesh=mesh, in_specs=(spec,), out_specs=(spec, spec), check_vma=False)
```

```python
import jax
import jax.numpy as jnp
import numpy as np
from jax import lax
from jax.experimental import pallas as pl
from jax.experimental.pallas import tpu as pltpu
from jax.sharding import PartitionSpec as P


R = 32
pair_first = (0, 0, 0, 0, 0, 1, 1, 1, 1, 2, 2, 2, 3, 3, 4)
pair_second = (0, 1, 2, 3, 4, 1, 2, 3, 4, 2, 3, 4, 3, 4, 4)
SCALE = 1.0 / (2 * R + 1)
H = 8
GROUPS = ((0,), (1,), (2,), (3,), (4,), (5,))
WINDOW = 2
RELAYED = (0,)
LAG = 1
F32 = jnp.float32
BF16 = jnp.bfloat16


VMEM = pl.BlockSpec(memory_space=pltpu.VMEM)
SMEM = pl.BlockSpec(memory_space=pltpu.SMEM)


def held(*arrays):
    return tuple(pltpu.with_memory_space_constraint(a, pltpu.VMEM) for a in arrays)


def components(ref, g, p, mask=None):
    values = [ref[g, c, p] for c in range(5)]
    if mask is not None:
        values = [v * mask for v in values]
    values += [values[a] * values[b] for a, b in zip(pair_first, pair_second)]
    return [v.astype(F32) for v in values]


def stream_kernel(inv_ref, edge_ref, lo_ref, own_ref, hi_ref, pack_ref, out_ref, low_ref, high_ref):
    mask_lo = jnp.full((2 * H, 128), edge_ref[0], F32).astype(BF16)
    mask_hi = jnp.full((2 * H, 128), edge_ref[1], F32).astype(BF16)

    @pl.loop(0, own_ref.shape[0])
    def _(g):
        def add(p, acc):
            lo = components(lo_ref, g, p, mask_lo)
            own = components(own_ref, g, p)
            both = [a + b for a, b in zip(lo, own)]
            return tuple(a + (b[:H] + b[H:]) for a, b in zip(acc, both))

        acc = lax.fori_loop(0, 16, add, tuple(jnp.zeros((H, 128), F32) for _ in range(20)))

        def slide(p, acc):
            inv_a, inv_b = inv_ref[2 * p], inv_ref[2 * p + 1]
            hi = components(hi_ref, g, p, mask_hi)
            lo = components(lo_ref, g, p, mask_lo)
            result = []
            for c in range(20):
                first = acc[c] + hi[c][:H]
                second = first + (hi[c][H:] - lo[c][:H])
                result.append(second - lo[c][H:])
                out_ref[g, c, p] = jnp.concatenate([first * inv_a, second * inv_b], axis=0).astype(BF16)
            return tuple(result)

        lax.fori_loop(0, 16, slide, acc)

        @pl.loop(0, 5, unroll=True)
        def _(b):
            part = pl.ds(4 * b, 4)
            block = out_ref[g, part].reshape(4, 4, 4, 2 * H, 128)
            rows = jnp.concatenate([block[:, :, q].reshape(32 * H, 128) for q in range(4)], axis=1)
            packed = jnp.dot(rows, pack_ref[...], preferred_element_type=F32).astype(BF16)
            low_ref[g, part] = packed[:, :128].reshape(4, 4, 2 * H, 128)
            high_ref[g, part] = packed[:, 128:].reshape(4, 4, 2 * H, 128)


def stream_filter(inv, edge, lo, own, hi, pack):
    n = own.shape[0]
    return pl.pallas_call(
        stream_kernel,
        in_specs=[SMEM, SMEM, VMEM, VMEM, VMEM, VMEM],
        out_specs=[VMEM, VMEM, VMEM],
        out_shape=[
            pltpu.VMEM((n, 20, 16, 2 * H, 128), BF16),
            pltpu.VMEM((n, 20, 4, 2 * H, 128), BF16),
            pltpu.VMEM((n, 20, 4, 2 * H, 128), BF16),
        ],
        compiler_params=pltpu.CompilerParams(vmem_limit_bytes=6 << 20),
        name="stream_filter",
    )(inv, edge, *held(lo, own, hi, pack))


def trans_kernel(own_ref, low_ref, high_ref, band_ref, out_ref):
    @pl.loop(0, own_ref.shape[0])
    def _(g):
        @pl.loop(0, 5)
        def _(b):
            part = pl.ds(4 * b, 4)
            own = own_ref[g, part].reshape(4, 4, 4, 2 * H, 128)
            low = low_ref[g, part].reshape(32 * H, 128)
            high = high_ref[g, part].reshape(32 * H, 128)
            for h in range(2):
                rows = jnp.concatenate(
                    [own[:, :, 2 * h].reshape(32 * H, 128), own[:, :, 2 * h + 1].reshape(32 * H, 128), low, high],
                    axis=1,
                )
                result = jnp.dot(rows, band_ref[h], preferred_element_type=F32) * SCALE
                result = result.astype(BF16).reshape(4, 4, 2 * H, 256)
                for s in range(4):
                    for e in range(2):
                        out_ref[g, part, 4 * s + 2 * h + e] = result[:, s, :, 128 * e : 128 * e + 128]


def trans_filter(own, low, high, band):
    return pl.pallas_call(
        trans_kernel,
        in_specs=[VMEM] * 4,
        out_specs=VMEM,
        out_shape=pltpu.VMEM(own.shape, BF16),
        compiler_params=pltpu.CompilerParams(vmem_limit_bytes=6 << 20),
        name="trans_filter",
    )(*held(own, low, high, band))


def span_kernel(band_ref, *refs):
    pieces, (filtered_ref, stress_ref, filtered_buf, stress_buf, sems) = refs[:-5], refs[-5:]
    rows = filtered_buf.shape[3]
    order = [(ref, g) for ref in pieces for g in range(ref.shape[0])]

    def copies(step, slot):
        x = step * 4
        return (
            pltpu.make_async_copy(filtered_buf.at[slot], filtered_ref.at[:, pl.ds(x, 4)], sems.at[0, slot]),
            pltpu.make_async_copy(stress_buf.at[slot], stress_ref.at[:, pl.ds(x, 4)], sems.at[1, slot]),
        )

    def step_body(step, _):
        slot = lax.rem(step, 2)

        @pl.when(step >= 2)
        def _():
            for copy in copies(step - 2, slot):
                copy.wait()

        def smooth(c):
            tile = jnp.concatenate(
                [jnp.concatenate([ref[g, c, 2 * step + i] for ref, g in order], axis=0) for i in range(2)], axis=1
            )
            return jnp.dot(band_ref[...], tile, preferred_element_type=F32) * SCALE

        def put(buf, c, value):
            for i in range(2):
                for e in range(2):
                    buf[slot, c, 2 * i + e] = value[rows * e : rows * e + rows, 128 * i : 128 * i + 128].astype(BF16)

        means = [smooth(c) for c in range(5)]
        for c in range(5):
            put(filtered_buf, c, means[c])
        for p in range(15):
            put(stress_buf, p, smooth(5 + p) - means[pair_first[p]] * means[pair_second[p]])
        for copy in copies(step, slot):
            copy.start()
        return 0

    lax.fori_loop(0, 8, step_body, 0)
    for step in (6, 7):
        for copy in copies(step, step % 2):
            copy.wait()


def span_filter(band, pieces, depth):
    anywhere = pl.BlockSpec(memory_space=pl.ANY)
    return pl.pallas_call(
        span_kernel,
        in_specs=[VMEM] * (1 + len(pieces)),
        out_specs=[anywhere, anywhere],
        out_shape=[
            jax.ShapeDtypeStruct((5, 32, depth, 128), BF16),
            jax.ShapeDtypeStruct((15, 32, depth, 128), BF16),
        ],
        scratch_shapes=[
            pltpu.VMEM((2, 5, 4, depth, 128), BF16),
            pltpu.VMEM((2, 15, 4, depth, 128), BF16),
            pltpu.SemaphoreType.DMA((2, 2)),
        ],
        compiler_params=pltpu.CompilerParams(vmem_limit_bytes=8 << 20),
        name="span_filter",
    )(*held(band, *pieces))


def inverse_norm(start, count, whole):
    cells = start + jnp.arange(count, dtype=jnp.int32)
    inside = jnp.minimum(cells + R, whole - 1) - jnp.maximum(cells - R, 0) + 1
    return 1.0 / inside.astype(F32)


def pack_matrix():
    k, n = np.indices((512, 256))
    return jnp.asarray((n % 128 // 32 == k // 128) & (k % 128 == n % 32 + 96 * (n // 128)), BF16)


def trans_band():
    h, k, n = np.indices((2, 512, 256))
    part, lane, e, target = k // 128, k % 128, n // 128, n % 128
    own = (part == e) & (np.abs(lane - target) <= R)
    mine = lane // 32 == 2 * h + e
    low = (part == 2) & mine & (np.abs(lane % 32 - 32 - target) <= R)
    high = (part == 3) & mine & (np.abs(lane % 32 + 128 - target) <= R)
    return jnp.asarray(own | low | high, BF16)


def span_band(odd, depth, outer, across):
    bands = []
    count = depth // H
    for core in range(2):
        starts = [depth - H * (k + 1) if core else H * k for k in range(count)]
        starts += [depth + H * k if core else -H * (k + 1) for k in outer]
        starts += [H * k - depth if core else 2 * depth - H * (k + 1) for k in across]
        position = np.array(starts)[:, None, None] + np.zeros((1, 2, 1), int) + np.arange(H)[None, None, :]
        half = np.zeros((len(starts), 1, 1), int) + np.arange(2)[None, :, None] + np.zeros((1, 1, H), int)
        position, half = position.reshape(1, -1), half.reshape(1, -1)
        e, row = np.indices((2, depth))
        e, row = e.reshape(-1, 1), row.reshape(-1, 1)
        bands.append((e == half) & (np.abs(position - row) <= R))
    return jnp.where(odd, jnp.asarray(bands[1], BF16), jnp.asarray(bands[0], BF16))


def plan(fields):
    depth_x, depth_y = fields.shape[1], fields.shape[2]
    nx, ny, nz = lax.axis_size("gx"), lax.axis_size("gy"), lax.axis_size("gz")
    place = lax.axis_index("gx")
    odd = lax.axis_index("gy") % 2 == 1
    inv = inverse_norm(place * depth_x, depth_x, depth_x * nx)
    edge = jnp.stack([place > 0, place < nx - 1]).astype(F32)
    outer_pieces = [k for i, group in enumerate(GROUPS) for _ in range(1 + (i in RELAYED)) for k in group if k < 4]
    across_pieces = [k for group in GROUPS for k in group if k >= 2]
    pack, band_z = pack_matrix(), trans_band()
    band_y = span_band(odd, depth_y, outer_pieces, across_pieces)

    def ring(n, by):
        return [(i, (i + by) % n) for i in range(n)]

    off_chip = [(i, (i - 1) % ny if i % 2 == 0 else (i + 1) % ny) for i in range(ny)]
    half = ny // 2
    ends = (0, half - 1, half, ny - 1)
    near = [(i, j) for i, j in off_chip if i not in ends]
    relay = {half - 1: 3, 0: 4, half: half + 4, ny - 1: half + 3}
    relay_out = list(relay.items())
    relay_in = [(relay[i], j) for i, j in off_chip if i in ends]
    on_chip = [(i, i + 1 if i % 2 == 0 else i - 1) for i in range(ny)]

    def after(value, *others):
        return lax.optimization_barrier((value, *others))[0]

    count = len(GROUPS)
    blocks, lows, highs = [], [], []

    def send_x(i, *others):
        parts = []
        for k in GROUPS[i]:
            start = jnp.where(odd, depth_y - H * (k + 1), H * k)
            part = lax.dynamic_slice_in_dim(fields, start, H, axis=2)
            parts.append(part.reshape(1, 5, 16, 2 * H, 128))
        block = jnp.concatenate(parts, axis=0)
        blocks.append(block)
        ahead = behind = block
        if i >= WINDOW:
            ahead = after(block, lows[i - WINDOW], *others)
            behind = after(block, highs[i - WINDOW], *others)
        lows.append(lax.ppermute(ahead, "gx", ring(nx, 1)))
        highs.append(lax.ppermute(behind, "gx", ring(nx, -1)))

    own, outer, across, waiting = [], [], [], []

    def finish_z(i, *others):
        streamed, from_low, from_high = waiting[i]
        if LAG:
            streamed = after(streamed, *others)
        done = trans_filter(streamed, from_low, from_high, band_z)
        own.append(done)
        if max(GROUPS[i]) < 4:
            outer.append(lax.ppermute(done, "gy", near if i in RELAYED else off_chip))
        if i in RELAYED:
            passed = lax.ppermute(done, "gy", relay_out)
            outer.append(lax.ppermute(passed, "gy", relay_in))
        if min(GROUPS[i]) >= 2:
            across.append(lax.ppermute(done, "gy", on_chip))

    for i in range(WINDOW):
        send_x(i)
    for i in range(count):
        last = own[-1:]
        if i + WINDOW < count:
            send_x(i + WINDOW, *last)
        streamed, low, high = stream_filter(inv, edge, lows[i], after(blocks[i], *last), highs[i], pack)
        from_low = lax.ppermute(high, "gz", ring(nz, 1))
        from_high = lax.ppermute(low, "gz", ring(nz, -1))
        waiting.append((streamed, from_low, from_high))
        if i >= LAG:
            finish_z(i - LAG, streamed)
    if LAG:
        finish_z(count - 1)
    return tuple(span_filter(band_y, own + outer + across, depth_y))


def solution(mesh):
    spec = P(None, "gx", "gy", "gz")
    return jax.shard_map(plan, mesh=mesh, in_specs=(spec,), out_specs=(spec, spec), check_vma=False)
```
